32 devices in a mesh: seq: 8 (over z, x), head: 4 (over y, core).
Axes of the slice: x: 2, y: 2, z: 4, core: 2. Of those that a mesh axis runs over, the one named last changes fastest.
Arguments:
- inputs: bfloat16 [8192, 4096], P('seq', 'head'), may hold values from -6 to 6
- out_grad: bfloat16 [8192, 4096], P('seq', 'head'), may hold values from -6 to 6
- b_proj: bfloat16 [8192, 128], P('seq'), may hold values from -0.75 to 0.75
- c_proj: bfloat16 [8192, 128], P('seq'), may hold values from -3 to 3
- step_raw: float32 [8192, 64], P('seq', 'head'), may hold values from -3 to 12
- log_rate: float32 [64], P('head'), may hold values from -7 to -1.7
- step_bias: float32 [64], P('head'), may hold values from -7 to -1.6
- skip_gain: float32 [64], P('head'), may hold values from 0.5 to 1.5
- saved_states: float32 [8, 64, 64, 128], P(None, 'seq', 'head'), may hold values from -1.5 to 1.5
- segment_slot: int32 [8], replicated, may hold values from 0 to 7, each once
Outputs:
- grad_inputs: bfloat16 [8192, 4096], P('seq', 'head')
- grad_step_raw: float32 [8192, 64], P('seq', 'head')
- grad_b: float32 [8192, 128], P(('seq', 'head'))
- grad_c: float32 [8192, 128], P(('seq', 'head'))
The draws below stay inside these ranges and needn't reach their ends.
Inputs may be any that keep to these rules, and one draw needn't show every extreme that they name: `segment_slot`: a permutation of the segments.
All inputs are finite; a program needn't handle non-finite values.
Results may differ from the reference program's by a relative error of at most 0.0012.
Values sent between devices are 32-bit elements; how exact they have to be, the bound alone decides.
A program may use at most 128 MiB of HBM per device.

```python
import jax
import jax.numpy as jnp
from jax import lax

H = 64
P_SIZE = 64
N = 128
SPAN = 256
TOK_DEV = 1024
SEGS = 8
TOKEN_COUNT = 8192


def head_rates(key):
    rate_key = jax.random.fold_in(key, 11)
    lowest = jnp.log(0.5 / TOKEN_COUNT)
    highest_rate = jnp.log(1.0 / 30.0)
    uniform_part = jax.random.uniform(rate_key, (H,), jnp.float32)
    log_value = lowest + uniform_part * (highest_rate - lowest)
    return jnp.exp(0.5 * log_value)


def draw_log_rate(key, part):
    return jnp.log(head_rates(key)).astype(jnp.float32)


def draw_step_bias(key, part):
    return jnp.log(jnp.expm1(head_rates(key))).astype(jnp.float32)


def draw_step_raw(key, part):
    private_random_key = jax.random.fold_in(key, 21)
    jitter_random_key, offset_random_key, spike_random_key = jax.random.split(private_random_key, 3)
    random_jitter = 0.5 * jnp.clip(jax.random.normal(jitter_random_key, (TOKEN_COUNT, H), jnp.float32), -3.0, 3.0)
    shifts = jax.random.uniform(offset_random_key, (SEGS, 1, H), jnp.float32, -0.7, 0.7)
    random_jitter = (random_jitter.reshape(SEGS, TOK_DEV, H) + shifts).reshape(TOKEN_COUNT, H)
    spike_positions = jax.random.randint(spike_random_key, (3,), 0, TOKEN_COUNT)
    spike_values = jnp.any(jnp.arange(TOKEN_COUNT)[:, None] == spike_positions[None, :], axis=1)
    return (random_jitter + 9.0 * spike_values[:, None].astype(jnp.float32)).astype(jnp.float32)


def shard_levels(own_key, extent, cuts, least, high):
    def one(position, shards_of):
        draws = jax.random.uniform(jax.random.fold_in(jax.random.fold_in(own_key, 6), position), (shards_of,), jnp.float32, least / len(cuts), high / len(cuts))
        return jnp.repeat(jnp.exp(draws), extent[position] // shards_of).reshape((-1,) + (1,) * (len(extent) - position - 1))

    gain = one(*cuts[0])
    for cut in cuts[1:]:
        gain = gain * one(*cut)
    return gain


def scatter_about(rng, shape, scale, bound, cuts=(), held_as=jnp.bfloat16):
    array = jax.random.normal(rng, shape, jnp.float32) * scale
    if len(cuts) > 0:
        array = shard_levels(rng, shape, cuts, -0.22, 0.18) * array
    return jnp.clip(array, min=-bound, max=bound).astype(held_as)


def setup_inputs(seed: int = 0) -> dict:
    streams_of = jax.random.split(jax.random.key(seed), 11)
    return {
        "inputs": scatter_about(streams_of[0], (TOKEN_COUNT, H * P_SIZE), 1.0, 6.0, ((0, 8), (1, 4))),
        "out_grad": scatter_about(streams_of[1], (TOKEN_COUNT, H * P_SIZE), 1.0, 6.0, ((0, 8), (1, 4))),
        "b_proj": scatter_about(streams_of[2], (TOKEN_COUNT, N), 0.125, 0.75, ((0, 8),)),
        "c_proj": scatter_about(streams_of[3], (TOKEN_COUNT, N), 0.5, 3.0, ((0, 8),)),
        "step_raw": draw_step_raw(jax.random.fold_in(streams_of[10], 71), 0),
        "log_rate": draw_log_rate(jax.random.fold_in(streams_of[10], 71), 0),
        "step_bias": draw_step_bias(jax.random.fold_in(streams_of[10], 71), 0),
        "skip_gain": jnp.clip(0.5 + 1.0 * jax.random.uniform(streams_of[7], (H,), jnp.float32) ** shard_levels(streams_of[7], (H,), ((0, 4),), -0.2, 0.2), 0.5, 1.5),
        "saved_states": scatter_about(streams_of[8], (SEGS, H, P_SIZE, N), 0.25, 1.5, ((1, 8), (2, 4)), jnp.float32),
        "segment_slot": jax.random.permutation(streams_of[9], SEGS).astype(jnp.int32),
    }


highest = lax.Precision.HIGHEST

def block_forward(carried, item, decay_rate, skip_gain, start_states, per_segment):
    block_index, input_block, b_block, c_block, step_block = item
    start = lax.dynamic_index_in_dim(start_states, block_index // per_segment, 0, keepdims=False)
    opening = block_index % per_segment == 0
    entering = jnp.where(opening, start + carried - lax.stop_gradient(carried), carried)
    log_decay = -decay_rate[None, :] * step_block
    cumulative = jnp.cumsum(log_decay, axis=0)
    positions = jnp.arange(cumulative.shape[0])
    lower_mask = positions[:, None] >= positions[None, :]
    spread = cumulative.T[:, :, None] - cumulative.T[:, None, :]
    decay = jnp.where(lower_mask, jnp.exp(jnp.where(lower_mask, spread, 0.0)), 0.0)
    intersection = jnp.einsum('tn,un->tu', c_block, b_block, precision=highest)
    weights = decay * intersection[None, :, :] * step_block.T[:, None, :]
    outputs = jnp.einsum('htu,uhp->thp', weights, input_block, precision=highest)
    outputs = outputs + jnp.exp(cumulative)[:, :, None] * jnp.einsum('hpn,tn->thp', entering, c_block, precision=highest)
    outputs = outputs + skip_gain[None, :, None] * input_block
    block_end = cumulative[-1]
    to_end = jnp.exp(block_end[None, :] - cumulative) * step_block
    leaving = jnp.exp(block_end)[:, None, None] * entering + jnp.einsum('uhp,un->hpn', input_block * to_end[:, :, None], b_block, precision=highest)
    return (leaving, outputs)

def reference(inputs, out_grad, b_proj, c_proj, step_raw, log_rate, step_bias, skip_gain, saved_states, segment_slot):
    seg_count = saved_states.shape[0]
    inverse_order = jnp.zeros((seg_count,), jnp.int32).at[segment_slot].set(jnp.arange(seg_count, dtype=jnp.int32))
    start_states = jnp.take(saved_states, inverse_order, axis=0)
    tok_count, state_dim = b_proj.shape
    head_count = step_raw.shape[1]
    head_width = inputs.shape[1] // head_count
    block_count = tok_count // SPAN
    per_segment = TOK_DEV // SPAN
    decay_rate = jnp.exp(log_rate)

    def forward(input_full, b_full, c_full, raw_full):
        step_size = jax.nn.softplus(raw_full + step_bias[None, :])

        def advance(carried, item):
            return block_forward(carried, item, decay_rate, skip_gain, start_states, per_segment)
        items = (jnp.arange(block_count, dtype=jnp.int32), input_full.reshape(block_count, SPAN, head_count, head_width), b_full.reshape(block_count, SPAN, state_dim), c_full.reshape(block_count, SPAN, state_dim), step_size.reshape(block_count, SPAN, head_count))
        initial = jnp.zeros((head_count, head_width, state_dim), jnp.float32)
        unused_end, outputs = lax.scan(jax.checkpoint(advance), initial, items)
        return outputs.reshape(tok_count, head_count * head_width)
    primals = (inputs.astype(jnp.float32), b_proj.astype(jnp.float32), c_proj.astype(jnp.float32), step_raw)
    unused_out, pullback = jax.vjp(forward, *primals)
    grad_inputs, grad_b, grad_c, grad_raw = pullback(out_grad.astype(jnp.float32))
    return (grad_inputs.astype(jnp.bfloat16), grad_raw, grad_b, grad_c)
```

```python
import functools
import math

import jax
import jax.numpy as jnp
from jax import lax
from jax.experimental import pallas as pl
from jax.experimental.pallas import tpu as pltpu
from jax.sharding import PartitionSpec as P

MESH = pl.DeviceIdType.MESH
LB = 128
f32, bf16 = jnp.float32, jnp.bfloat16
LOG2E = math.log2(math.e)


def mm(a, b):
    return jnp.dot(a, b, preferred_element_type=f32)


def mm_nt(a, b):
    return lax.dot_general(a, b, (((1,), (1,)), ((), ())), preferred_element_type=f32)


def split(v):
    hi = v.astype(bf16)
    return hi, (v - hi.astype(f32)).astype(bf16)


def mm2(v, b):
    hi, lo = split(v)
    return mm(hi, b) + mm(lo, b)


def mm_exact(tri, v):
    hi = v.astype(bf16)
    rest = v - hi.astype(f32)
    mid = rest.astype(bf16)
    low = (rest - mid.astype(f32)).astype(bf16)
    return mm(tri, hi) + mm(tri, mid) + mm(tri, low)


def kernel(
    S,
    HD,
    x_ref,
    dy_ref,
    b_ref,
    c_ref,
    raw_ref,
    rate_ref,
    bias_ref,
    skip_ref,
    start,
    gin_ref,
    graw_ref,
    gb_ref,
    gc_ref,
    dys,
    xs,
    dsx,
    decx,
    gpart,
    fpart,
    states,
    adj,
    ecol,
    crow,
    dtc,
    yrow,
    yint,
    gbacc,
    gcacc,
    dsum,
    xrecv,
    zsend,
    zrecv,
    bsend,
    rown,
    rback,
    gbrecv,
    gcrecv,
    expm,
    redm,
    x_send,
    x_recv,
    z_send,
    z_recv,
    b_send,
    b_recv,
    gb_send,
    gb_recv,
    gc_send,
    gc_recv,
):
    T, HP = x_ref.shape
    heads = raw_ref.shape[1]
    width = HP // heads
    nstate = b_ref.shape[1]
    nblk = T // LB
    pairs = HP // 128
    per = 128 // width
    half = pairs // 2
    s = lax.axis_index("seq")
    hd = lax.axis_index("head")
    xx = lax.rem(s, 2)
    zz = s // 2
    Z = S // 2
    rows_out = T // HD

    barrier = pltpu.get_barrier_semaphore()

    def greet(i, _):
        a, b = i // HD, lax.rem(i, HD)

        @pl.when(jnp.logical_or(a != s, b != hd))
        def _():
            pl.semaphore_signal(barrier, inc=1, device_id=(a, b), device_id_type=MESH)

        return 0

    lax.fori_loop(0, S * HD, greet, 0)

    @pl.when(zz == Z - 1)
    def _():
        zrecv[...] = jnp.zeros(zrecv.shape, f32)

    lane_head = lax.broadcasted_iota(jnp.int32, (heads, HP), 1) // width
    expm[...] = (lane_head == lax.broadcasted_iota(jnp.int32, (heads, HP), 0)).astype(f32).astype(bf16)
    row_head = lax.broadcasted_iota(jnp.int32, (HP, heads), 0) // width
    redm[...] = (row_head == lax.broadcasted_iota(jnp.int32, (HP, heads), 1)).astype(f32).astype(bf16)

    iu = lax.broadcasted_iota(jnp.int32, (LB, LB), 0)
    iv = lax.broadcasted_iota(jnp.int32, (LB, LB), 1)
    tril = (iu >= iv).astype(f32).astype(bf16)
    triu = (iu <= iv).astype(f32).astype(bf16)

    rate = jnp.exp(rate_ref[...])
    bias = bias_ref[...]

    def prep(c, _):
        rows = pl.ds(pl.multiple_of(c * LB, LB), LB)
        raw = raw_ref[rows, :] + bias
        z = jnp.exp(-jnp.abs(raw))
        small = z * (1.0 - z * (0.5 - z * (1.0 / 3.0 - 0.25 * z)))
        dt = jnp.maximum(raw, 0.0) + jnp.where(z < 0.02, small, jnp.log(1.0 + z))
        cum = mm_exact(tril, dt * (-LOG2E * rate))
        end = cum[LB - 1 : LB, :]
        growth = jnp.exp2(cum)
        ds = dt * jnp.exp2(end - cum)
        dtc[rows, :] = dt
        ecol[rows, :] = cum - LOG2E * jnp.log(dt)
        crow[c] = cum.T
        gx = mm2(growth, expm[...])
        decx[c] = gx[LB - 1 : LB, :]
        dx = mm2(ds, expm[...])
        dsx[rows, :] = dx
        hi, lo = split(dy_ref[rows, :].astype(f32) * gx)
        dys[c, pl.ds(0, LB), :] = hi
        dys[c, pl.ds(LB, LB), :] = lo
        ct = c_ref[rows, :].astype(f32).T.astype(bf16)
        gpart[c] = mm(jnp.concatenate([ct, ct], axis=1), dys[c])
        return 0

    lax.fori_loop(0, nblk, prep, 0)

    for j in range(pairs):
        cols = pl.ds(128 * j, 128)

        def to_left(i, carry, cols=cols):
            c = nblk - 1 - i
            total, decay = carry
            d = decx[c, :, cols]
            return gpart[c, :, cols] + d * total, decay * d

        total, decay = lax.fori_loop(
            0, nblk, to_left, (jnp.zeros((nstate, 128), f32), jnp.ones((1, 128), f32))
        )
        dsum[j, pl.ds(0, nstate), :] = total
        dsum[j, pl.ds(nstate, 8), :] = jnp.broadcast_to(decay, (8, 128))

    pl.semaphore_wait(barrier, S * HD - 1)

    def x_copy(k):
        return pltpu.make_async_remote_copy(
            src_ref=dsum.at[(1 - xx) * half + k],
            dst_ref=xrecv.at[k],
            send_sem=x_send.at[k],
            recv_sem=x_recv.at[k],
            device_id=(s + 1 - 2 * xx, hd),
            device_id_type=MESH,
        )

    for k in range(half):
        x_copy(k).start()

    def z_copy(k):
        return pltpu.make_async_remote_copy(
            src_ref=zsend.at[k],
            dst_ref=zrecv.at[k],
            send_sem=z_send.at[k],
            recv_sem=z_recv.at[k],
            device_id=(s - 2, hd),
            device_id_type=MESH,
        )

    def b_copy(k):
        return pltpu.make_async_remote_copy(
            src_ref=bsend.at[k],
            dst_ref=rback.at[k],
            send_sem=b_send.at[k],
            recv_sem=b_recv.at[k],
            device_id=(s + 1 - 2 * xx, hd),
            device_id_type=MESH,
        )

    def link(k):
        x_copy(k).wait_recv()

        @pl.when(zz < Z - 1)
        def _():
            z_copy(k).wait_recv()

        own = xx * half + k
        first = xx == 0
        m_sum = dsum[own, pl.ds(0, nstate), :]
        m_dec = dsum[own, pl.ds(nstate, 1), :]
        t_sum = xrecv[k, pl.ds(0, nstate), :]
        t_dec = xrecv[k, pl.ds(nstate, 1), :]
        incoming = zrecv[k]
        later = jnp.where(first, t_sum, m_sum)
        later_dec = jnp.where(first, t_dec, m_dec)
        early = jnp.where(first, m_sum, t_sum)
        early_dec = jnp.where(first, m_dec, t_dec)
        middle = later + later_dec * incoming
        zsend[k] = early + early_dec * middle

        @pl.when(zz > 0)
        def _():
            z_copy(k).start()

        rown[k] = jnp.where(first, middle, incoming)
        bsend[k] = jnp.where(first, incoming, middle)
        b_copy(k).start()

    masks = [
        (lax.broadcasted_iota(jnp.int32, (1, 128), 1) // width == a).astype(f32).astype(bf16)
        for a in range(per)
    ]
    reach = iv >= iu

    def intra(c, _):
        rows = pl.ds(pl.multiple_of(c * LB, LB), LB)
        b = b_ref[rows, :]
        cc = c_ref[rows, :]
        cbt = mm_nt(b, cc)
        ec = ecol[rows, :]
        head_total = jnp.zeros((LB, LB), f32)
        for j in range(pairs):
            cols = slice(128 * j, 128 * j + 128)
            xp = x_ref[rows, cols]
            dyp = dy_ref[rows, cols]
            dyst = jnp.concatenate([dyp * m for m in masks], axis=0)
            dots = mm_nt(xp, dyst)
            his, los = [], []
            for a in range(per):
                h = per * j + a
                spread = crow[c, pl.ds(h, 1), :] - ec[:, h : h + 1]
                decay = jnp.exp2(jnp.where(reach, spread, -1e30))
                hi, lo = split(decay * cbt)
                his.append(hi)
                los.append(lo)
                pair_in = dots[:, LB * a : LB * a + LB] * decay
                head_total = head_total + pair_in
                yrow[c, pl.ds(h, 1), :] = jnp.sum(pair_in * cbt, axis=0, keepdims=True)
            both = jnp.concatenate(
                [jnp.concatenate(his, axis=1), jnp.concatenate(los, axis=1)], axis=0
            )
            res = mm(both, dyst)
            adj[rows, cols] = res[:LB] + res[LB:]
        gbacc[rows, :] = mm2(head_total, cc)
        gcacc[rows, :] = mm2(head_total.T, b)
        dx = dsx[rows, :]
        hi, lo = split(x_ref[rows, :].astype(f32) * dx)
        xs[c, pl.ds(0, LB), :] = hi
        xs[c, pl.ds(LB, LB), :] = lo
        bt = b.astype(f32).T.astype(bf16)
        fpart[c] = mm(jnp.concatenate([bt, bt], axis=1), xs[c])
        return 0

    lax.fori_loop(0, nblk, intra, 0)

    for j in range(pairs):
        block = start[per * j : per * j + per].reshape(128, nstate)
        states[0, :, 128 * j : 128 * j + 128] = block.T

    def forward(c, _):
        rows = pl.ds(pl.multiple_of(c * LB, LB), LB)
        cc = c_ref[rows, :]
        state = states[c]
        states[c + 1] = decx[c] * state + fpart[c]
        hi, lo = split(state)
        st2 = jnp.concatenate([hi, lo], axis=0)
        sc = mm(jnp.concatenate([cc, cc], axis=1), st2)
        d_hi = dys[c, pl.ds(0, LB), :]
        d_lo = dys[c, pl.ds(LB, LB), :]
        r1 = mm_nt(d_hi, st2)
        gcacc[rows, :] = (
            gcacc[rows, :] + r1[:, :nstate] + r1[:, nstate:] + mm_nt(d_lo, hi)
        )
        prod = (d_hi.astype(f32) + d_lo.astype(f32)) * sc
        yint[rows, :] = mm2(prod, redm[...])
        return 0

    lax.fori_loop(0, nblk, forward, 0)

    def send_out(acc, recv, ssem, rsem, d):
        to = lax.rem(hd + d, HD)
        return pltpu.make_async_remote_copy(
            src_ref=acc.at[pl.ds(pl.multiple_of(to * rows_out, 8), rows_out), :],
            dst_ref=recv.at[d - 1],
            send_sem=ssem.at[d - 1],
            recv_sem=rsem.at[d - 1],
            device_id=(s, to),
            device_id_type=MESH,
        )

    for d in range(1, HD):
        send_out(gcacc, gcrecv, gc_send, gc_recv, d).start()

    for k in range(half):
        link(k)

    hi = skip_ref[...].astype(bf16)
    rem1 = skip_ref[...] - hi.astype(f32)
    mid = rem1.astype(bf16)
    skipx = mm(hi, expm[...]) + mm(mid, expm[...])

    own_half = jnp.concatenate([rown[k] for k in range(half)], axis=1)
    for k in range(half):
        b_copy(k).wait_recv()
    other_half = jnp.concatenate([rback[k] for k in range(half)], axis=1)
    adjoint = jnp.concatenate(
        [jnp.where(xx == 0, own_half, other_half), jnp.where(xx == 0, other_half, own_half)],
        axis=1,
    )

    per_out = nblk // HD

    states_g = fpart
    states_g[0] = adjoint

    def back_block(c):
        rows = pl.ds(pl.multiple_of(c * LB, LB), LB)
        b = b_ref[rows, :]
        g = states_g[0]
        through = jnp.sum(g * states[c + 1], axis=0, keepdims=True)
        hi, lo = split(g)
        g2 = jnp.concatenate([hi, lo], axis=0)
        bg = mm(jnp.concatenate([b, b], axis=1), g2)
        ab = adj[rows, :] + dsx[rows, :] * bg
        dyf = dy_ref[rows, :].astype(f32)
        gin_ref[rows, :] = (ab + skipx * dyf).astype(bf16)
        zz_sum = mm2(x_ref[rows, :].astype(f32) * ab, redm[...])
        x_hi = xs[c, pl.ds(0, LB), :]
        x_lo = xs[c, pl.ds(LB, LB), :]
        r1 = mm_nt(x_hi, g2)
        gbacc[rows, :] = gbacc[rows, :] + r1[:, :nstate] + r1[:, nstate:] + mm_nt(x_lo, hi)
        w_end = mm2(jnp.broadcast_to(through, (8, HP)), redm[...])[0:1, :]
        y_sum = yrow[c].T + yint[rows, :]
        w = w_end + mm_exact(triu, y_sum - zz_sum)
        raw = raw_ref[rows, :] + bias
        graw_ref[rows, :] = (zz_sum / dtc[rows, :] - rate * w) / (1.0 + jnp.exp(-raw))
        states_g[0] = gpart[c] + decx[c] * g

    def back(i, _):
        j = HD - 1 - i

        def inner(q, _):
            back_block(j * per_out + per_out - 1 - q)
            return 0

        lax.fori_loop(0, per_out, inner, 0)

        return 0

    lax.fori_loop(0, HD, back, 0)
    for d in range(1, HD):
        send_out(gbacc, gbrecv, gb_send, gb_recv, d).start()

    own_rows = pl.ds(pl.multiple_of(hd * rows_out, 8), rows_out)
    for acc, recv, ssem, rsem, out in (
        (gcacc, gcrecv, gc_send, gc_recv, gc_ref),
        (gbacc, gbrecv, gb_send, gb_recv, gb_ref),
    ):
        total = acc[own_rows, :]
        for d in range(1, HD):
            send_out(acc, recv, ssem, rsem, d).wait_recv()
            total = total + recv[d - 1]
        out[...] = total

    for d in range(1, HD):
        send_out(gcacc, gcrecv, gc_send, gc_recv, d).wait_send()
        send_out(gbacc, gbrecv, gb_send, gb_recv, d).wait_send()

    for k in range(half):
        x_copy(k).wait_send()
        b_copy(k).wait_send()

        @pl.when(zz > 0)
        def _(k=k):
            z_copy(k).wait_send()


def on_device(S, HD, inputs, out_grad, b, c, raw, log_rate, bias, skip, saved, slot):
    T, HP = inputs.shape
    heads = raw.shape[1]
    width = HP // heads
    N = b.shape[1]
    nblk = T // LB
    pairs = HP // 128
    half = pairs // 2
    inverse = jnp.zeros((S,), jnp.int32).at[slot].set(jnp.arange(S, dtype=jnp.int32))
    ordered = jnp.take(saved, inverse, axis=0)
    start = lax.all_to_all(
        lax.all_to_all(ordered, "seq", split_axis=0, concat_axis=1, tiled=True),
        "head",
        split_axis=1,
        concat_axis=2,
        tiled=True,
    )[0]
    vm = pl.BlockSpec(memory_space=pltpu.VMEM)
    dma = lambda n: pltpu.SemaphoreType.DMA((n,))
    V = pltpu.VMEM
    return pl.pallas_call(
        functools.partial(kernel, S, HD),
        out_shape=(
            jax.ShapeDtypeStruct((T, HP), bf16),
            jax.ShapeDtypeStruct((T, heads), f32),
            jax.ShapeDtypeStruct((T // HD, N), f32),
            jax.ShapeDtypeStruct((T // HD, N), f32),
        ),
        in_specs=[vm] * 9,
        out_specs=(vm, vm, vm, vm),
        scratch_shapes=[
            V((nblk, 2 * LB, HP), bf16),
            V((nblk, 2 * LB, HP), bf16),
            V((T, HP), f32),
            V((nblk, 1, HP), f32),
            V((nblk, N, HP), f32),
            V((nblk, N, HP), f32),
            V((nblk + 1, N, HP), f32),
            V((T, HP), f32),
            V((T, heads), f32),
            V((nblk, heads, LB), f32),
            V((T, heads), f32),
            V((nblk, heads, LB), f32),
            V((T, heads), f32),
            V((T, N), f32),
            V((T, N), f32),
            V((pairs, N + 8, 128), f32),
            V((half, N + 8, 128), f32),
            V((half, N, 128), f32),
            V((half, N, 128), f32),
            V((half, N, 128), f32),
            V((half, N, 128), f32),
            V((half, N, 128), f32),
            V((HD - 1, T // HD, N), f32),
            V((HD - 1, T // HD, N), f32),
            V((heads, HP), bf16),
            V((HP, heads), bf16),
            dma(half),
            dma(half),
            dma(half),
            dma(half),
            dma(half),
            dma(half),
            dma(HD - 1),
            dma(HD - 1),
            dma(HD - 1),
            dma(HD - 1),
        ],
        compiler_params=pltpu.CompilerParams(
            collective_id=0, has_side_effects=True, vmem_limit_bytes=60 * 1024 * 1024
        ),
        name="ssm_backward",
    )(
        inputs,
        out_grad,
        b,
        c,
        raw,
        log_rate.reshape(1, heads),
        bias.reshape(1, heads),
        skip.reshape(1, heads),
        start,
    )


def solution(mesh):
    placed = (
        P("seq", "head"),
        P("seq", "head"),
        P("seq", None),
        P("seq", None),
        P("seq", "head"),
        P("head"),
        P("head"),
        P("head"),
        P(None, "seq", "head", None),
        P(),
    )
    return jax.shard_map(
        functools.partial(on_device, mesh.shape["seq"], mesh.shape["head"]),
        mesh=mesh,
        in_specs=placed,
        out_specs=(
            P("seq", "head"),
            P("seq", "head"),
            P(("seq", "head"), None),
            P(("seq", "head"), None),
        ),
        check_vma=False,
    )
```

```python
import functools
import math

import jax
import jax.numpy as jnp
from jax import lax
from jax.experimental import pallas as pl
from jax.experimental.pallas import tpu as pltpu
from jax.sharding import PartitionSpec as P

MESH = pl.DeviceIdType.MESH
STAGES = 4
LB = 128
f32, bf16 = jnp.float32, jnp.bfloat16
LOG2E = math.log2(math.e)


def mm(a, b):
    return jnp.dot(a, b, preferred_element_type=f32)


def mm_nt(a, b):
    return lax.dot_general(a, b, (((1,), (1,)), ((), ())), preferred_element_type=f32)


def split(v):
    hi = v.astype(bf16)
    return hi, (v - hi.astype(f32)).astype(bf16)


def mm2(v, b):
    hi, lo = split(v)
    return mm(hi, b) + mm(lo, b)


def mm_exact(tri, v):
    hi = v.astype(bf16)
    rest = v - hi.astype(f32)
    mid = rest.astype(bf16)
    low = (rest - mid.astype(f32)).astype(bf16)
    return mm(tri, hi) + mm(tri, mid) + mm(tri, low)


def kernel(
    S,
    HD,
    x_ref,
    dy_ref,
    b_ref,
    c_ref,
    raw_ref,
    rate_ref,
    bias_ref,
    skip_ref,
    start,
    gin_ref,
    graw_ref,
    gb_ref,
    gc_ref,
    dys,
    xs,
    dsx,
    decx,
    gpart,
    fpart,
    states,
    adj,
    ecol,
    crow,
    dtc,
    yrow,
    yint,
    gbacc,
    gcacc,
    dsum,
    xrecv,
    zsend,
    zrecv,
    bsend,
    rown,
    rback,
    gbrecv,
    gcrecv,
    expm,
    redm,
    x_send,
    x_recv,
    z_send,
    z_recv,
    b_send,
    b_recv,
    gb_send,
    gb_recv,
    gc_send,
    gc_recv,
):
    T, HP = x_ref.shape
    heads = raw_ref.shape[1]
    width = HP // heads
    nstate = b_ref.shape[1]
    nblk = T // LB
    pairs = HP // 128
    per = 128 // width
    half = pairs // 2
    s = lax.axis_index("seq")
    hd = lax.axis_index("head")
    xx = lax.rem(s, 2)
    zz = s // 2
    Z = S // 2
    rows_out = T // HD

    barrier = pltpu.get_barrier_semaphore()

    def greet(i, _):
        a, b = i // HD, lax.rem(i, HD)

        @pl.when(jnp.logical_or(a != s, b != hd))
        def _():
            pl.semaphore_signal(barrier, inc=1, device_id=(a, b), device_id_type=MESH)

        return 0

    lax.fori_loop(0, S * HD, greet, 0)

    @pl.when(zz == Z - 1)
    def _():
        zrecv[...] = jnp.zeros(zrecv.shape, f32)

    lane_head = lax.broadcasted_iota(jnp.int32, (heads, HP), 1) // width
    expm[...] = (lane_head == lax.broadcasted_iota(jnp.int32, (heads, HP), 0)).astype(f32).astype(bf16)
    row_head = lax.broadcasted_iota(jnp.int32, (HP, heads), 0) // width
    redm[...] = (row_head == lax.broadcasted_iota(jnp.int32, (HP, heads), 1)).astype(f32).astype(bf16)

    iu = lax.broadcasted_iota(jnp.int32, (LB, LB), 0)
    iv = lax.broadcasted_iota(jnp.int32, (LB, LB), 1)
    tril = (iu >= iv).astype(f32).astype(bf16)
    triu = (iu <= iv).astype(f32).astype(bf16)

    rate = jnp.exp(rate_ref[...])
    bias = bias_ref[...]

    def prep(c, _):
        rows = pl.ds(pl.multiple_of(c * LB, LB), LB)
        raw = raw_ref[rows, :] + bias
        z = jnp.exp(-jnp.abs(raw))
        small = z * (1.0 - z * (0.5 - z * (1.0 / 3.0 - 0.25 * z)))
        dt = jnp.maximum(raw, 0.0) + jnp.where(z < 0.02, small, jnp.log(1.0 + z))
        cum = mm_exact(tril, dt * (-LOG2E * rate))
        end = cum[LB - 1 : LB, :]
        growth = jnp.exp2(cum)
        ds = dt * jnp.exp2(end - cum)
        dtc[rows, :] = dt
        ecol[rows, :] = cum - LOG2E * jnp.log(dt)
        crow[c] = cum.T
        gx = mm2(growth, expm[...])
        decx[c] = gx[LB - 1 : LB, :]
        dx = mm2(ds, expm[...])
        dsx[rows, :] = dx
        hi, lo = split(dy_ref[rows, :].astype(f32) * gx)
        dys[c, pl.ds(0, LB), :] = hi
        dys[c, pl.ds(LB, LB), :] = lo
        ct = c_ref[rows, :].astype(f32).T.astype(bf16)
        gpart[c] = mm(jnp.concatenate([ct, ct], axis=1), dys[c])
        return 0

    lax.fori_loop(0, nblk, prep, 0)

    for j in range(pairs):
        cols = pl.ds(128 * j, 128)

        def to_left(i, carry, cols=cols):
            c = nblk - 1 - i
            total, decay = carry
            d = decx[c, :, cols]
            return gpart[c, :, cols] + d * total, decay * d

        total, decay = lax.fori_loop(
            0, nblk, to_left, (jnp.zeros((nstate, 128), f32), jnp.ones((1, 128), f32))
        )
        dsum[j, pl.ds(0, nstate), :] = total
        dsum[j, pl.ds(nstate, 8), :] = jnp.broadcast_to(decay, (8, 128))

    pl.semaphore_wait(barrier, S * HD - 1)

    def x_copy(k):
        return pltpu.make_async_remote_copy(
            src_ref=dsum.at[(1 - xx) * half + k],
            dst_ref=xrecv.at[k],
            send_sem=x_send.at[k],
            recv_sem=x_recv.at[k],
            device_id=(s + 1 - 2 * xx, hd),
            device_id_type=MESH,
        )

    for k in range(half):
        x_copy(k).start()

    def z_copy(k):
        return pltpu.make_async_remote_copy(
            src_ref=zsend.at[k],
            dst_ref=zrecv.at[k],
            send_sem=z_send.at[k],
            recv_sem=z_recv.at[k],
            device_id=(s - 2, hd),
            device_id_type=MESH,
        )

    def b_copy(k):
        return pltpu.make_async_remote_copy(
            src_ref=bsend.at[k],
            dst_ref=rback.at[k],
            send_sem=b_send.at[k],
            recv_sem=b_recv.at[k],
            device_id=(s + 1 - 2 * xx, hd),
            device_id_type=MESH,
        )

    def link(k):
        x_copy(k).wait_recv()

        @pl.when(zz < Z - 1)
        def _():
            z_copy(k).wait_recv()

        own = xx * half + k
        first = xx == 0
        m_sum = dsum[own, pl.ds(0, nstate), :]
        m_dec = dsum[own, pl.ds(nstate, 1), :]
        t_sum = xrecv[k, pl.ds(0, nstate), :]
        t_dec = xrecv[k, pl.ds(nstate, 1), :]
        incoming = zrecv[k]
        later = jnp.where(first, t_sum, m_sum)
        later_dec = jnp.where(first, t_dec, m_dec)
        early = jnp.where(first, m_sum, t_sum)
        early_dec = jnp.where(first, m_dec, t_dec)
        middle = later + later_dec * incoming
        zsend[k] = early + early_dec * middle

        @pl.when(zz > 0)
        def _():
            z_copy(k).start()

        rown[k] = jnp.where(first, middle, incoming)
        bsend[k] = jnp.where(first, incoming, middle)
        b_copy(k).start()

    def stage(q):
        ready = zz == Z - 1 - q if q < STAGES - 1 else zz <= Z - STAGES

        @pl.when(ready)
        def _():
            for k in range(half):
                link(k)

    masks = [
        (lax.broadcasted_iota(jnp.int32, (1, 128), 1) // width == a).astype(f32).astype(bf16)
        for a in range(per)
    ]
    reach = iv >= iu

    def intra(c, _):
        rows = pl.ds(pl.multiple_of(c * LB, LB), LB)
        b = b_ref[rows, :]
        cc = c_ref[rows, :]
        cbt = mm_nt(b, cc)
        ec = ecol[rows, :]
        head_total = jnp.zeros((LB, LB), f32)
        for j in range(pairs):
            cols = slice(128 * j, 128 * j + 128)
            xp = x_ref[rows, cols]
            dyp = dy_ref[rows, cols]
            dyst = jnp.concatenate([dyp * m for m in masks], axis=0)
            dots = mm_nt(xp, dyst)
            his, los = [], []
            for a in range(per):
                h = per * j + a
                spread = crow[c, pl.ds(h, 1), :] - ec[:, h : h + 1]
                decay = jnp.exp2(jnp.where(reach, spread, -1e30))
                hi, lo = split(decay * cbt)
                his.append(hi)
                los.append(lo)
                pair_in = dots[:, LB * a : LB * a + LB] * decay
                head_total = head_total + pair_in
                yrow[c, pl.ds(h, 1), :] = jnp.sum(pair_in * cbt, axis=0, keepdims=True)
            both = jnp.concatenate(
                [jnp.concatenate(his, axis=1), jnp.concatenate(los, axis=1)], axis=0
            )
            res = mm(both, dyst)
            adj[rows, cols] = res[:LB] + res[LB:]
        gbacc[rows, :] = mm2(head_total, cc)
        gcacc[rows, :] = mm2(head_total.T, b)
        dx = dsx[rows, :]
        hi, lo = split(x_ref[rows, :].astype(f32) * dx)
        xs[c, pl.ds(0, LB), :] = hi
        xs[c, pl.ds(LB, LB), :] = lo
        bt = b.astype(f32).T.astype(bf16)
        fpart[c] = mm(jnp.concatenate([bt, bt], axis=1), xs[c])
        return 0

    lax.fori_loop(0, nblk // 2 + 1, intra, 0)
    stage(0)
    lax.fori_loop(nblk // 2 + 1, nblk, intra, 0)
    stage(1)

    for j in range(pairs):
        block = start[per * j : per * j + per].reshape(128, nstate)
        states[0, :, 128 * j : 128 * j + 128] = block.T

    def forward(c, _):
        rows = pl.ds(pl.multiple_of(c * LB, LB), LB)
        cc = c_ref[rows, :]
        state = states[c]
        states[c + 1] = decx[c] * state + fpart[c]
        hi, lo = split(state)
        st2 = jnp.concatenate([hi, lo], axis=0)
        sc = mm(jnp.concatenate([cc, cc], axis=1), st2)
        d_hi = dys[c, pl.ds(0, LB), :]
        d_lo = dys[c, pl.ds(LB, LB), :]
        r1 = mm_nt(d_hi, st2)
        gcacc[rows, :] = (
            gcacc[rows, :] + r1[:, :nstate] + r1[:, nstate:] + mm_nt(d_lo, hi)
        )
        prod = (d_hi.astype(f32) + d_lo.astype(f32)) * sc
        yint[rows, :] = mm2(prod, redm[...])
        return 0

    lax.fori_loop(0, nblk // 2, forward, 0)
    stage(2)
    lax.fori_loop(nblk // 2, nblk, forward, 0)
    stage(3)

    def send_out(acc, recv, ssem, rsem, d):
        to = lax.rem(hd + d, HD)
        return pltpu.make_async_remote_copy(
            src_ref=acc.at[pl.ds(pl.multiple_of(to * rows_out, 8), rows_out), :],
            dst_ref=recv.at[d - 1],
            send_sem=ssem.at[d - 1],
            recv_sem=rsem.at[d - 1],
            device_id=(s, to),
            device_id_type=MESH,
        )

    for d in range(1, HD):
        send_out(gcacc, gcrecv, gc_send, gc_recv, d).start()

    hi = skip_ref[...].astype(bf16)
    rem1 = skip_ref[...] - hi.astype(f32)
    mid = rem1.astype(bf16)
    skipx = mm(hi, expm[...]) + mm(mid, expm[...])

    own_half = jnp.concatenate([rown[k] for k in range(half)], axis=1)
    for k in range(half):
        b_copy(k).wait_recv()
    other_half = jnp.concatenate([rback[k] for k in range(half)], axis=1)
    adjoint = jnp.concatenate(
        [jnp.where(xx == 0, own_half, other_half), jnp.where(xx == 0, other_half, own_half)],
        axis=1,
    )

    per_out = nblk // HD

    states_g = fpart
    states_g[0] = adjoint

    def back_block(c):
        rows = pl.ds(pl.multiple_of(c * LB, LB), LB)
        b = b_ref[rows, :]
        g = states_g[0]
        through = jnp.sum(g * states[c + 1], axis=0, keepdims=True)
        hi, lo = split(g)
        g2 = jnp.concatenate([hi, lo], axis=0)
        bg = mm(jnp.concatenate([b, b], axis=1), g2)
        ab = adj[rows, :] + dsx[rows, :] * bg
        dyf = dy_ref[rows, :].astype(f32)
        gin_ref[rows, :] = (ab + skipx * dyf).astype(bf16)
        zz_sum = mm2(x_ref[rows, :].astype(f32) * ab, redm[...])
        x_hi = xs[c, pl.ds(0, LB), :]
        x_lo = xs[c, pl.ds(LB, LB), :]
        r1 = mm_nt(x_hi, g2)
        gbacc[rows, :] = gbacc[rows, :] + r1[:, :nstate] + r1[:, nstate:] + mm_nt(x_lo, hi)
        w_end = mm2(jnp.broadcast_to(through, (8, HP)), redm[...])[0:1, :]
        y_sum = yrow[c].T + yint[rows, :]
        w = w_end + mm_exact(triu, y_sum - zz_sum)
        raw = raw_ref[rows, :] + bias
        graw_ref[rows, :] = (zz_sum / dtc[rows, :] - rate * w) / (1.0 + jnp.exp(-raw))
        states_g[0] = gpart[c] + decx[c] * g

    def back(i, _):
        j = HD - 1 - i

        def inner(q, _):
            back_block(j * per_out + per_out - 1 - q)
            return 0

        lax.fori_loop(0, per_out, inner, 0)

        return 0

    lax.fori_loop(0, HD, back, 0)
    for d in range(1, HD):
        send_out(gbacc, gbrecv, gb_send, gb_recv, d).start()

    own_rows = pl.ds(pl.multiple_of(hd * rows_out, 8), rows_out)
    for acc, recv, ssem, rsem, out in (
        (gcacc, gcrecv, gc_send, gc_recv, gc_ref),
        (gbacc, gbrecv, gb_send, gb_recv, gb_ref),
    ):
        total = acc[own_rows, :]
        for d in range(1, HD):
            send_out(acc, recv, ssem, rsem, d).wait_recv()
            total = total + recv[d - 1]
        out[...] = total

    for d in range(1, HD):
        send_out(gcacc, gcrecv, gc_send, gc_recv, d).wait_send()
        send_out(gbacc, gbrecv, gb_send, gb_recv, d).wait_send()

    for k in range(half):
        x_copy(k).wait_send()
        b_copy(k).wait_send()

        @pl.when(zz > 0)
        def _(k=k):
            z_copy(k).wait_send()


def on_device(S, HD, inputs, out_grad, b, c, raw, log_rate, bias, skip, saved, slot):
    T, HP = inputs.shape
    heads = raw.shape[1]
    width = HP // heads
    N = b.shape[1]
    nblk = T // LB
    pairs = HP // 128
    half = pairs // 2
    inverse = jnp.zeros((S,), jnp.int32).at[slot].set(jnp.arange(S, dtype=jnp.int32))
    ordered = jnp.take(saved, inverse, axis=0)
    start = lax.all_to_all(
        lax.all_to_all(ordered, "seq", split_axis=0, concat_axis=1, tiled=True),
        "head",
        split_axis=1,
        concat_axis=2,
        tiled=True,
    )[0]
    vm = pl.BlockSpec(memory_space=pltpu.VMEM)
    dma = lambda n: pltpu.SemaphoreType.DMA((n,))
    V = pltpu.VMEM
    return pl.pallas_call(
        functools.partial(kernel, S, HD),
        out_shape=(
            jax.ShapeDtypeStruct((T, HP), bf16),
            jax.ShapeDtypeStruct((T, heads), f32),
            jax.ShapeDtypeStruct((T // HD, N), f32),
            jax.ShapeDtypeStruct((T // HD, N), f32),
        ),
        in_specs=[vm] * 9,
        out_specs=(vm, vm, vm, vm),
        scratch_shapes=[
            V((nblk, 2 * LB, HP), bf16),
            V((nblk, 2 * LB, HP), bf16),
            V((T, HP), f32),
            V((nblk, 1, HP), f32),
            V((nblk, N, HP), f32),
            V((nblk, N, HP), f32),
            V((nblk + 1, N, HP), f32),
            V((T, HP), f32),
            V((T, heads), f32),
            V((nblk, heads, LB), f32),
            V((T, heads), f32),
            V((nblk, heads, LB), f32),
            V((T, heads), f32),
            V((T, N), f32),
            V((T, N), f32),
            V((pairs, N + 8, 128), f32),
            V((half, N + 8, 128), f32),
            V((half, N, 128), f32),
            V((half, N, 128), f32),
            V((half, N, 128), f32),
            V((half, N, 128), f32),
            V((half, N, 128), f32),
            V((HD - 1, T // HD, N), f32),
            V((HD - 1, T // HD, N), f32),
            V((heads, HP), bf16),
            V((HP, heads), bf16),
            dma(half),
            dma(half),
            dma(half),
            dma(half),
            dma(half),
            dma(half),
            dma(HD - 1),
            dma(HD - 1),
            dma(HD - 1),
            dma(HD - 1),
        ],
        compiler_params=pltpu.CompilerParams(
            collective_id=0, has_side_effects=True, vmem_limit_bytes=60 * 1024 * 1024
        ),
        name="ssm_backward",
    )(
        inputs,
        out_grad,
        b,
        c,
        raw,
        log_rate.reshape(1, heads),
        bias.reshape(1, heads),
        skip.reshape(1, heads),
        start,
    )


def solution(mesh):
    placed = (
        P("seq", "head"),
        P("seq", "head"),
        P("seq", None),
        P("seq", None),
        P("seq", "head"),
        P("head"),
        P("head"),
        P("head"),
        P(None, "seq", "head", None),
        P(),
    )
    return jax.shard_map(
        functools.partial(on_device, mesh.shape["seq"], mesh.shape["head"]),
        mesh=mesh,
        in_specs=placed,
        out_specs=(
            P("seq", "head"),
            P("seq", "head"),
            P(("seq", "head"), None),
            P(("seq", "head"), None),
        ),
        check_vma=False,
    )
```
